32 devices in a mesh: groups: 2 (over y), pages: 4 (over z), patches: 4 (over x, core).
Axes of the slice: x: 2, y: 2, z: 4, core: 2. Of those that a mesh axis runs over, the one named last changes fastest.
Arguments:
- queries: bfloat16 [16, 32, 128], P(('groups', 'pages'), 'patches'), parts along dimension 0, may hold values from -6 to 6
- gallery: bfloat16 [640, 1024, 128], P(('groups', 'pages'), 'patches'), parts along dimension 0, may hold values from -0.5 to 0.5
- page_rows: int32 [640], P('groups'), parts along dimension 0, may hold values from 0 to 319, as said below
- candidates: int32 [16, 32], P(('groups', 'pages')), parts along dimension 0, may hold values from 0 to 319, as said below
Outputs:
- scores: float32 [16, 32], P(('groups', 'pages')), parts along dimension 0
The draws below stay inside these ranges and needn't reach their ends.
There are 2 independent parts, one for each index of `groups`. The reference program is written for one: setup_inputs(seed, part) draws one part's arguments, and reference() takes and returns one part's arrays. A program takes and returns all parts, laid end to end along the dimension named above; each array names one. Nothing has to cross between parts.
Inputs may be any that keep to these rules, and one draw needn't show every extreme that they name: A permutation: page id c is stored at row page_rows[c] of gallery, which lies on pages index page_rows[c] // 80. Each query's 32 page ids are distinct. The 2 queries of one pages index have at most 48 candidates stored on one pages index, and in every draw some pages index stores exactly 48 candidates of the queries of every pages index.
All inputs are finite; a program needn't handle non-finite values.
Results may differ from the reference program's by a relative error of at most 0.0003.
Values may be sent and summed in bfloat16 or wider, within the bound.
A program may use at most 64 MiB of HBM per device.

```python
import jax
import jax.numpy as jnp
from jax import lax

DIM = 128
PATCH = 1024
QT = 32
CAND_OWN = 8
NQ_DEV = 2
PG_DEV = 80
CAND = 32
NQ = 8
PAGES = 320
N_PAGES = 4


def candidate_plan(key):
    owners = N_PAGES
    spots = 4 * CAND_OWN
    page_rows = jax.random.permutation(jax.random.fold_in(key, 101), PAGES).astype(jnp.int32)
    row_to_page = jnp.argsort(page_rows).astype(jnp.int32)
    hottest = jax.random.randint(jax.random.fold_in(key, 102), (), 0, owners)
    offsets = jax.random.randint(jax.random.fold_in(key, 103), (owners, NQ_DEV), 0, CAND_OWN)
    query_index = jnp.arange(NQ_DEV)
    signs = jnp.where(query_index % 2 == 0, 1, -1)
    signs = jnp.where((query_index % 2 == 0) & (query_index == NQ_DEV - 1), 0, signs)
    hot_counts = 3 * CAND_OWN + signs[None, :] * offsets[:, query_index // 2]
    limits = jax.random.randint(jax.random.fold_in(key, 104), (owners, NQ_DEV, owners), CAND_OWN, 3 * CAND_OWN + 1)
    is_hot = jnp.arange(owners) == hottest
    limits = jnp.where(is_hot[None, None, :], 0, limits)
    slot_index = jnp.arange(3 * CAND_OWN)
    open_slots = slot_index[None, None, None, :] < limits[..., None]
    noise = jax.random.randint(jax.random.fold_in(key, 105), open_slots.shape, 0, 2 ** 20)
    priority = jnp.where(open_slots, 2 ** 21, 0) + noise
    flat_priority = priority.reshape(owners, NQ_DEV, owners * 3 * CAND_OWN)
    ordering = jnp.argsort(-flat_priority, axis=-1)
    position = jnp.argsort(ordering, axis=-1)
    needed = CAND - hot_counts
    chosen = position < needed[..., None]
    counts = jnp.sum(chosen.reshape(owners, NQ_DEV, owners, 3 * CAND_OWN).astype(jnp.int32), axis=-1)
    counts = counts + jnp.where(is_hot[None, None, :], hot_counts[..., None], 0)
    local_noise = jax.random.randint(jax.random.fold_in(key, 106), (owners, NQ_DEV, owners, PG_DEV), 0, 2 ** 30)
    local_order = jnp.argsort(local_noise, axis=-1)[..., :spots].astype(jnp.int32)
    spot_index = jnp.arange(spots)
    usable = spot_index[None, None, None, :] < counts[..., None]
    storage = jnp.arange(owners, dtype=jnp.int32)[None, None, :, None] * PG_DEV + local_order
    flat_storage = storage.reshape(owners, NQ_DEV, owners * spots)
    flat_usable = usable.reshape(owners, NQ_DEV, owners * spots)
    shuffle = jax.random.randint(jax.random.fold_in(key, 107), flat_storage.shape, 0, 2 ** 20)
    sort_keys = jnp.where(flat_usable, 0, 2 ** 21) + shuffle
    taken = jnp.argsort(sort_keys, axis=-1)[..., :CAND]
    picked = jnp.take_along_axis(flat_storage, taken, axis=-1)
    candidates = row_to_page[picked].reshape(owners * NQ_DEV, CAND).astype(jnp.int32)
    return (page_rows, candidates)


def draw_page_rows(key, part):
    return candidate_plan(key)[0]


def draw_candidates(key, part):
    return candidate_plan(key)[1]


def level_of(rng, shape, shards, low, top_value):
    factor_of = 1.0
    for dim, parts in shards:
        heights = jax.random.uniform(jax.random.fold_in(jax.random.fold_in(rng, 6), dim), (parts,), jnp.float32, low / len(shards), top_value / len(shards))
        factor_of = factor_of * jnp.repeat(jnp.exp(heights), shape[dim] // parts).reshape((-1,) + (1,) * (len(shape) - 1 - dim))
    return factor_of


def centred(stream_key, extent, scale, reach, split=(), kind=jnp.bfloat16):
    drawn = jax.random.normal(stream_key, extent, jnp.float32) * scale
    if len(split) > 0:
        drawn = level_of(stream_key, extent, split, -0.22, 0.18) * drawn
    return jnp.clip(drawn, min=-reach, max=reach).astype(kind)


def setup_inputs(seed: int = 0, part: int = 0) -> dict:
    arg_keys = jax.random.split(jax.random.key(seed), 5)
    own_keys = jax.random.split(jax.random.fold_in(arg_keys[4], part), 5)
    queries = centred(own_keys[0], (NQ, QT, DIM), 1.0, 6.0, ((0, 4), (1, 4)))
    gallery = centred(own_keys[1], (PAGES, PATCH, DIM), DIM ** -0.5, 0.5, ((0, 4), (1, 4)))
    page_rows = draw_page_rows(jax.random.fold_in(jax.random.fold_in(arg_keys[4], part), 71), part)
    candidates = draw_candidates(jax.random.fold_in(jax.random.fold_in(arg_keys[4], part), 71), part)
    return dict(queries=queries, gallery=gallery, page_rows=page_rows, candidates=candidates)


def reference(queries, gallery, page_rows, candidates):
    rows = jnp.take(page_rows, candidates, axis=0).astype(jnp.int32)

    def per_query(item):
        tokens, row_ids = item
        pages = jnp.take(gallery, row_ids, axis=0).astype(jnp.float32)
        sims = jnp.einsum("td,cpd->ctp", tokens.astype(jnp.float32), pages, precision=lax.Precision.HIGHEST)
        return jnp.mean(jnp.max(sims, axis=2), axis=1)

    return lax.map(per_query, (queries, rows))
```

```python
import functools

import jax
import jax.numpy as jnp
from jax import lax
from jax.experimental import pallas as pl
from jax.experimental.pallas import tpu as pltpu
from jax.sharding import PartitionSpec as P

MESH = pl.DeviceIdType.MESH


def up(n, m):
    return -(-n // m) * m


def repeat(n, body):
    if n <= 16:
        for k in range(n):
            body(k)
    else:

        @pl.loop(0, n)
        def _(k):
            body(k)


def to_column(row):
    n = row.shape[1]
    eye = lax.broadcasted_iota(jnp.int32, (n, n), 0) == lax.broadcasted_iota(jnp.int32, (n, n), 1)
    return jnp.sum(jnp.where(eye, row, 0.0), axis=1, keepdims=True)


def to_row(column):
    n = column.shape[0]
    eye = lax.broadcasted_iota(jnp.int32, (n, n), 0) == lax.broadcasted_iota(jnp.int32, (n, n), 1)
    return jnp.sum(jnp.where(eye, column, 0.0), axis=0, keepdims=True)


def top_row(sims):
    rows, width = sims.shape
    chains = 4
    if rows % (8 * chains) == 0:
        sims = jnp.max(sims.reshape(rows // (8 * chains), chains, 8, width), axis=0)
        sims = jnp.maximum(jnp.maximum(sims[0], sims[1]), jnp.maximum(sims[2], sims[3]))
    return jnp.max(sims, axis=0, keepdims=True)


def kernel(
    dims,
    q_hbm,
    g_ref,
    rows_hbm,
    cand_hbm,
    out_ref,
    q_ref,
    rows_ref,
    cand_ref,
    q_all,
    g_buf,
    lists,
    slots,
    best,
    best_in,
    send,
    arrived,
    g_sem,
    a_sem,
    q_out,
    q_in,
    l_own,
    l_out,
    l_in,
    b_out,
    b_in,
    s_out,
    s_in,
):
    n_pages, n_patches, nq, tokens = dims
    devices = n_pages * n_patches
    page_count = g_ref.shape[0]
    pairs = best.shape[1]
    lanes = lists.shape[2]
    me_g = lax.axis_index("groups")
    me_p = lax.axis_index("pages")
    me_j = lax.axis_index("patches")
    finisher = lax.rem(me_j, 2) == 1
    finishers = n_patches // 2

    def there(p, j):
        return (me_g, p, j)

    def holder(k):
        k = jnp.int32(k)
        below = me_p
        above = n_pages - 1 - me_p
        both = 2 * jnp.minimum(below, above)
        longest = jnp.maximum(below, above)
        single = longest - both // 2
        first = jnp.where(below > above, k, n_pages - 1 - k)
        rest = k - single
        alternating = jnp.where(
            lax.rem(rest, 2) == 0, both // 2 - rest // 2, -(both // 2 - rest // 2)
        )
        return jnp.where(k < single, first, me_p + alternating)

    def group(step):
        if isinstance(step, int) and step == 0:
            return me_p
        if isinstance(step, int) and step == 1:
            return jnp.where(me_p > 0, me_p - 1, 1)
        k = step - 2
        return jnp.where(k < me_p - 1, k, k + 2)

    def peer(k):
        if isinstance(k, int):
            p = holder(k // n_patches) if k < devices - n_patches else me_p
            spread = k % n_patches if k < devices - n_patches else k % n_patches + 1
        else:
            far = k < devices - n_patches
            p = jnp.where(far, holder(k // n_patches), me_p)
            spread = jnp.where(far, lax.rem(k, n_patches), lax.rem(k, n_patches) + 1)
        return p, lax.rem(me_j + n_patches - spread, n_patches)

    barrier = pltpu.get_barrier_semaphore()

    def greet(k):
        p, j = peer(k)
        pl.semaphore_signal(barrier, inc=1, device_id=there(p, j), device_id_type=MESH)

    repeat(devices - 1, greet)
    small = [
        pltpu.make_async_copy(source, target, a_sem.at[k])
        for k, (source, target) in enumerate(
            ((q_hbm, q_ref), (cand_hbm, cand_ref), (rows_hbm, rows_ref))
        )
    ]
    for copy in small:
        copy.start()
    gallery_copy = pltpu.make_async_copy(g_ref, g_buf, g_sem)
    gallery_copy.start()
    send[...] = jnp.zeros_like(send)
    for copy in small:
        copy.wait()

    q_all[me_p, me_j] = q_ref[...]
    page_rows = rows_ref[...].astype(jnp.float32).reshape(1, -1)
    columns = []
    for q in range(nq):
        wanted = to_column(cand_ref[q : q + 1, :].astype(jnp.float32))
        ids = lax.broadcasted_iota(jnp.int32, (wanted.shape[0], page_rows.shape[1]), 1)
        hit = ids.astype(jnp.float32) == wanted
        columns.append(jnp.sum(jnp.where(hit, page_rows, 0.0), axis=1, keepdims=True))
    row = jnp.concatenate(columns, axis=0)
    held_by = jnp.zeros_like(row)
    for h in range(1, n_pages):
        held_by = held_by + jnp.where(row >= float(h * page_count), 1.0, 0.0)
    local = row - held_by * float(page_count)
    n = row.shape[0]
    earlier = lax.broadcasted_iota(jnp.int32, (n, n), 1) < lax.broadcasted_iota(jnp.int32, (n, n), 0)
    same = to_row(held_by) == held_by
    place = jnp.sum(jnp.where(earlier & same, 1.0, 0.0), axis=1, keepdims=True)
    key = held_by * float(lanes) + place
    lane = lax.broadcasted_iota(jnp.int32, (n, lanes), 1)

    def make_list(h):
        chosen = key == (lane + h * lanes).astype(jnp.float32)
        found = jnp.sum(jnp.where(chosen, local, 0.0), axis=0, keepdims=True).astype(jnp.int32)
        lists[h] = jnp.clip(found, 0, page_count - 1)

    repeat(n_pages, make_list)
    own_list = pltpu.make_async_copy(lists.at[me_p], slots.at[me_p], l_own)
    own_list.start()

    pl.semaphore_wait(barrier, devices - 1)

    def send_queries(k):
        p, j = peer(k)
        pltpu.make_async_remote_copy(
            src_ref=q_ref,
            dst_ref=q_all.at[me_p, me_j],
            send_sem=q_out,
            recv_sem=q_in.at[me_p],
            device_id=there(p, j),
            device_id_type=MESH,
        ).start()

    def send_list(k):
        p = holder(k)
        pltpu.make_async_remote_copy(
            src_ref=lists.at[p],
            dst_ref=slots.at[me_p],
            send_sem=l_out,
            recv_sem=l_in.at[me_p],
            device_id=there(p, me_j),
            device_id_type=MESH,
        ).start()

    repeat(n_pages - 1, send_list)
    repeat(devices - 1, send_queries)

    def maxima(g):
        rows = q_all[g].reshape(n_patches * q_all.shape[2], q_all.shape[3])
        none = jnp.zeros_like(rows)
        weights = jnp.concatenate(
            [jnp.concatenate([rows, none], axis=1), jnp.concatenate([none, rows], axis=1)], axis=0
        )
        for k in range(pairs):
            pair = jnp.concatenate([g_buf[slots[g, 0, k]], g_buf[slots[g, 0, pairs + k]]], axis=1)
            sims = lax.dot_general(
                pair, weights, (((1,), (1,)), ((), ())), preferred_element_type=jnp.float32
            )
            best[g, k : k + 1, :] = top_row(sims)

    def best_copy(g, j):
        return pltpu.make_async_remote_copy(
            src_ref=best.at[g],
            dst_ref=best_in.at[g, me_j],
            send_sem=b_out,
            recv_sem=b_in.at[g],
            device_id=there(me_p, j),
            device_id_type=MESH,
        )

    def send_best(g):
        for k in range(1, finishers):
            best_copy(g, lax.rem(me_j // 2 + k, finishers) * 2 + 1).start()

        @pl.when(jnp.logical_not(finisher))
        def _():
            best_copy(g, me_j + 1).start()

    width = best.shape[2]
    own_tokens = tokens // n_patches
    column = lax.broadcasted_iota(jnp.int32, (send.shape[1], width), 1)
    query = lax.broadcasted_iota(jnp.int32, (send.shape[1], width), 0)
    position = column // own_tokens
    named = position // (n_patches * nq) * nq + position % nq
    mean = jnp.where(named == query, 1.0 / tokens, 0.0)

    def score_copy(g, k):
        return pltpu.make_async_remote_copy(
            src_ref=send.at[g],
            dst_ref=arrived.at[me_p],
            send_sem=s_out,
            recv_sem=s_in.at[me_p],
            device_id=there(g, me_j - k),
            device_id_type=MESH,
        )

    def finish(step):
        g = group(step)
        others = best_in.at[g, pl.ds(0, n_patches - 1)]
        pltpu.make_async_copy(others, others, b_in.at[g]).wait()
        total = best[g]
        for k in range(1, n_patches):
            total = jnp.maximum(total, best_in[g, lax.rem(me_j + k, n_patches)])
        scores = lax.dot_general(
            mean,
            total,
            (((1,), (1,)), ((), ())),
            precision=lax.Precision.HIGHEST,
            preferred_element_type=jnp.float32,
        )
        send[g, :, :pairs] = scores
        score_copy(g, 1).start()
        if isinstance(step, int) and step == 0:
            arrived[me_p] = send[g]
        else:
            score_copy(g, 0).start()

    def take(step):
        g = group(step)
        if isinstance(step, int) and step == 0:
            some = q_all.at[g, pl.ds(0, n_patches - 1)]
            pltpu.make_async_copy(some, some, q_in.at[g]).wait()
            own_list.wait()
            gallery_copy.wait()
        else:
            some = q_all.at[g]
            pltpu.make_async_copy(some, some, q_in.at[g]).wait()
            pltpu.make_async_copy(slots.at[g], slots.at[g], l_in.at[g]).wait()
        maxima(g)
        send_best(g)

    def maybe_finish(step):
        @pl.when(finisher)
        def _():
            finish(step)

    lag = min(2, n_pages)
    head = min(n_pages, 4)
    for step in range(head):
        take(step)
        if step >= lag:
            maybe_finish(step - lag)
    if head < n_pages:
        for step in range(head - lag, head):
            maybe_finish(step)

        @pl.loop(head, n_pages)
        def _(step):
            take(step)
            maybe_finish(step)

    else:
        for step in range(n_pages - lag, n_pages):
            maybe_finish(step)

    spots = lax.broadcasted_iota(jnp.int32, (cand_ref.shape[1], lanes), 1)
    cands = cand_ref.shape[1]

    def pick(h, picked):
        found = []
        for q in range(nq):
            mine = key[q * cands : (q + 1) * cands]
            total = picked[q]
            for half in range(2):
                spot = (spots + (h * lanes + half * pairs)).astype(jnp.float32)
                hit = (mine == spot) & (spots < pairs)
                total = total + jnp.where(hit, arrived[h, half * nq + q : half * nq + q + 1, :], 0.0)
            found.append(total)
        return tuple(found)

    def wait_scores(h):
        pltpu.make_async_copy(arrived.at[h], arrived.at[h], s_in.at[h]).wait()

    @pl.when(jnp.logical_not(finisher))
    def _():
        wait_scores(me_p)

    picked = tuple(jnp.zeros((cands, lanes), jnp.float32) for _ in range(nq))
    picked = pick(me_p, picked)
    if n_pages <= 16:
        for k in reversed(range(n_pages - 1)):
            wait_scores(holder(k))
            picked = pick(holder(k), picked)
    else:

        def later(k, picked):
            wait_scores(holder(k))
            return pick(holder(k), picked)

        picked = lax.fori_loop(0, n_pages - 1, later, picked)
    for q in range(nq):
        out_ref[q : q + 1, :] = to_row(jnp.sum(picked[q], axis=1, keepdims=True))

    def drain(k):
        pltpu.make_async_copy(q_ref, q_ref, q_out).wait()

    rest = q_all.at[pl.ds(0, n_pages - 1)]
    pltpu.make_async_copy(rest, rest, q_out).wait()
    rest = q_all.at[0, pl.ds(0, n_patches - 1)]
    pltpu.make_async_copy(rest, rest, q_out).wait()
    rest = lists.at[pl.ds(0, n_pages - 1)]
    pltpu.make_async_copy(rest, rest, l_out).wait()
    if finishers > 1:
        rest = best_in.at[:, pl.ds(0, finishers - 1)]
        pltpu.make_async_copy(rest, rest, b_out).wait()

    @pl.when(jnp.logical_not(finisher))
    def _():
        pltpu.make_async_copy(best, best, b_out).wait()

    @pl.when(finisher)
    def _():
        pltpu.make_async_copy(arrived, arrived, s_out).wait()
        rest = arrived.at[pl.ds(0, n_pages - 1)]
        pltpu.make_async_copy(rest, rest, s_out).wait()


def body(queries, gallery, page_rows, candidates):
    nq, own_tokens, dim = queries.shape
    n_pages, n_patches = lax.axis_size("pages"), lax.axis_size("patches")
    most = 3 * nq * candidates.shape[1] // n_pages
    pairs = up(up(most, 2) // 2, 8)
    lanes = up(2 * pairs, 128)
    width = 2 * n_patches * nq * own_tokens
    vmem = pl.BlockSpec(memory_space=pltpu.VMEM)
    dma = pltpu.SemaphoreType.DMA
    return pl.pallas_call(
        functools.partial(kernel, (n_pages, n_patches, nq, own_tokens * n_patches)),
        out_shape=pltpu.VMEM(candidates.shape, jnp.float32),
        in_specs=[pl.BlockSpec(memory_space=pl.ANY)] * 4,
        out_specs=vmem,
        scratch_shapes=[
            pltpu.VMEM((nq * own_tokens, dim), jnp.bfloat16),
            pltpu.VMEM(page_rows.shape, jnp.int32),
            pltpu.VMEM(candidates.shape, jnp.int32),
            pltpu.VMEM((n_pages, n_patches, nq * own_tokens, dim), jnp.bfloat16),
            pltpu.VMEM(gallery.shape, jnp.bfloat16),
            pltpu.VMEM((n_pages, 1, lanes), jnp.int32),
            pltpu.SMEM((n_pages, 1, lanes), jnp.int32),
            pltpu.VMEM((n_pages, pairs, width), jnp.float32),
            pltpu.VMEM((n_pages, n_patches, pairs, width), jnp.float32),
            pltpu.VMEM((n_pages, up(2 * nq, 8), lanes), jnp.float32),
            pltpu.VMEM((n_pages, up(2 * nq, 8), lanes), jnp.float32),
            dma,
            dma((3,)),
            dma,
            dma((n_pages,)),
            dma,
            dma,
            dma((n_pages,)),
            dma,
            dma((n_pages,)),
            dma,
            dma((n_pages,)),
        ],
        compiler_params=pltpu.CompilerParams(collective_id=0, has_side_effects=True),
    )(
        queries.reshape(nq * own_tokens, dim),
        gallery,
        page_rows,
        candidates,
    )


def solution(mesh):
    in_specs = (
        P(("groups", "pages"), "patches", None),
        P(("groups", "pages"), "patches", None),
        P("groups"),
        P(("groups", "pages"), None),
    )
    out_specs = P(("groups", "pages"), None)
    return jax.shard_map(body, mesh=mesh, in_specs=in_specs, out_specs=out_specs, check_vma=False)
```

```python
import functools

import jax
import jax.numpy as jnp
from jax import lax
from jax.experimental import pallas as pl
from jax.experimental.pallas import tpu as pltpu
from jax.sharding import PartitionSpec as P

MESH = pl.DeviceIdType.MESH


def up(n, m):
    return -(-n // m) * m


def repeat(n, body):
    if n <= 16:
        for k in range(n):
            body(k)
    else:

        @pl.loop(0, n)
        def _(k):
            body(k)


def to_column(row):
    n = row.shape[1]
    eye = lax.broadcasted_iota(jnp.int32, (n, n), 0) == lax.broadcasted_iota(jnp.int32, (n, n), 1)
    return jnp.sum(jnp.where(eye, row, 0.0), axis=1, keepdims=True)


def to_row(column):
    n = column.shape[0]
    eye = lax.broadcasted_iota(jnp.int32, (n, n), 0) == lax.broadcasted_iota(jnp.int32, (n, n), 1)
    return jnp.sum(jnp.where(eye, column, 0.0), axis=0, keepdims=True)


def top_row(sims):
    rows, width = sims.shape
    chains = 4
    if rows % (8 * chains) == 0:
        sims = jnp.max(sims.reshape(rows // (8 * chains), chains, 8, width), axis=0)
        sims = jnp.maximum(jnp.maximum(sims[0], sims[1]), jnp.maximum(sims[2], sims[3]))
    return jnp.max(sims, axis=0, keepdims=True)


def kernel(
    dims,
    q_hbm,
    g_ref,
    rows_hbm,
    cand_hbm,
    out_ref,
    q_ref,
    rows_ref,
    cand_ref,
    q_all,
    g_buf,
    lists,
    slots,
    best,
    best_in,
    direct_in,
    send,
    arrived,
    g_sem,
    a_sem,
    q_out,
    q_in,
    l_own,
    l_out,
    l_in,
    b_out,
    b_in,
    s_out,
    s_in,
    d_out,
    d_in,
    ready,
):
    n_pages, n_patches, nq, tokens = dims
    devices = n_pages * n_patches
    page_count = g_ref.shape[0]
    pairs = best.shape[1]
    lanes = lists.shape[2]
    me_g = lax.axis_index("groups")
    me_p = lax.axis_index("pages")
    me_j = lax.axis_index("patches")
    finisher = lax.rem(me_j, 2) == 1
    finishers = n_patches // 2
    direct = (me_p == 0) & (me_j < 2)

    def there(p, j):
        return (me_g, p, j)

    def holder(k):
        k = jnp.int32(k)
        below = me_p
        above = n_pages - 1 - me_p
        both = 2 * jnp.minimum(below, above)
        longest = jnp.maximum(below, above)
        single = longest - both // 2
        first = jnp.where(below > above, k, n_pages - 1 - k)
        rest = k - single
        alternating = jnp.where(
            lax.rem(rest, 2) == 0, both // 2 - rest // 2, -(both // 2 - rest // 2)
        )
        return jnp.where(k < single, first, me_p + alternating)

    def group(step):
        step = jnp.int32(step)
        low = jnp.where(step == 0, me_p, jnp.where(step <= me_p, step - 1, step))
        high = jnp.where(step < me_p, me_p - 1 - step, jnp.where(step == n_pages - 1, me_p, step + 1))
        return jnp.where(me_p > 2, high, low)

    barrier = pltpu.get_barrier_semaphore()

    def greet(p, j):
        pl.semaphore_signal(barrier, inc=1, device_id=there(p, j), device_id_type=MESH)

    def across(p, first, act):
        for k in range(first, n_patches):
            act(p, lax.rem(me_j + k, n_patches))

    def above(act):
        def one(k):
            @pl.when(n_pages - 1 - k > me_p)
            def _():
                act(n_pages - 1 - k)

        repeat(n_pages - 1, one)

    def below(act):
        def one(k):
            @pl.when(k < me_p)
            def _():
                act(k)

        repeat(n_pages - 1, one)

    across(me_p, 1, greet)
    above(lambda p: across(p, 0, greet))
    small = [
        pltpu.make_async_copy(source, target, a_sem.at[k])
        for k, (source, target) in enumerate(
            ((q_hbm, q_ref), (cand_hbm, cand_ref), (rows_hbm, rows_ref))
        )
    ]
    for copy in small:
        copy.start()
    gallery_copy = pltpu.make_async_copy(g_ref, g_buf, g_sem)
    gallery_copy.start()
    send[...] = jnp.zeros_like(send)
    for copy in small:
        copy.wait()

    q_all[me_p, me_j] = q_ref[...]
    page_rows = rows_ref[...].astype(jnp.float32).reshape(1, -1)
    columns = []
    for q in range(nq):
        wanted = to_column(cand_ref[q : q + 1, :].astype(jnp.float32))
        ids = lax.broadcasted_iota(jnp.int32, (wanted.shape[0], page_rows.shape[1]), 1)
        hit = ids.astype(jnp.float32) == wanted
        columns.append(jnp.sum(jnp.where(hit, page_rows, 0.0), axis=1, keepdims=True))
    row = jnp.concatenate(columns, axis=0)
    held_by = jnp.zeros_like(row)
    for h in range(1, n_pages):
        held_by = held_by + jnp.where(row >= float(h * page_count), 1.0, 0.0)
    local = row - held_by * float(page_count)
    n = row.shape[0]
    earlier = lax.broadcasted_iota(jnp.int32, (n, n), 1) < lax.broadcasted_iota(jnp.int32, (n, n), 0)
    same = to_row(held_by) == held_by
    place = jnp.sum(jnp.where(earlier & same, 1.0, 0.0), axis=1, keepdims=True)
    key = held_by * float(lanes) + place
    lane = lax.broadcasted_iota(jnp.int32, (n, lanes), 1)

    def make_list(h):
        chosen = key == (lane + h * lanes).astype(jnp.float32)
        found = jnp.sum(jnp.where(chosen, local, 0.0), axis=0, keepdims=True).astype(jnp.int32)
        lists[h] = jnp.clip(found, 0, page_count - 1)

    repeat(n_pages, make_list)
    own_list = pltpu.make_async_copy(lists.at[me_p], slots.at[me_p], l_own)
    own_list.start()

    pl.semaphore_wait(barrier, n_patches - 1 + n_patches * me_p)

    def announce(p):
        for k in range(2):
            pl.semaphore_signal(
                ready.at[me_p], inc=1, device_id=there(p, me_j - k), device_id_type=MESH
            )

    @pl.when(finisher)
    def _():
        below(announce)

    def send_queries(p, j):
        pltpu.make_async_remote_copy(
            src_ref=q_ref,
            dst_ref=q_all.at[me_p, me_j],
            send_sem=q_out,
            recv_sem=q_in.at[me_p],
            device_id=there(p, j),
            device_id_type=MESH,
        ).start()

    def send_to(p):
        across(p, 0, send_queries)
        pltpu.make_async_remote_copy(
            src_ref=lists.at[p],
            dst_ref=slots.at[me_p],
            send_sem=l_out,
            recv_sem=l_in.at[me_p],
            device_id=there(p, me_j),
            device_id_type=MESH,
        ).start()

    across(me_p, 1, send_queries)
    below(send_to)

    def send_above(k):
        @pl.when(k + 1 > me_p)
        def _():
            pl.semaphore_wait(ready.at[k + 1], 1)
            send_to(k + 1)

    repeat(n_pages - 1, send_above)

    def maxima(g):
        rows = q_all[g].reshape(n_patches * q_all.shape[2], q_all.shape[3])
        none = jnp.zeros_like(rows)
        weights = jnp.concatenate(
            [jnp.concatenate([rows, none], axis=1), jnp.concatenate([none, rows], axis=1)], axis=0
        )
        for k in range(pairs):
            pair = jnp.concatenate([g_buf[slots[g, 0, k]], g_buf[slots[g, 0, pairs + k]]], axis=1)
            sims = lax.dot_general(
                pair, weights, (((1,), (1,)), ((), ())), preferred_element_type=jnp.float32
            )
            best[g, k : k + 1, :] = top_row(sims)

    def best_copy(g, j):
        return pltpu.make_async_remote_copy(
            src_ref=best.at[g],
            dst_ref=best_in.at[g, me_j],
            send_sem=b_out,
            recv_sem=b_in.at[g],
            device_id=there(me_p, j),
            device_id_type=MESH,
        )

    def direct_copy(j):
        return pltpu.make_async_remote_copy(
            src_ref=best.at[0],
            dst_ref=direct_in.at[me_p, me_j],
            send_sem=d_out,
            recv_sem=d_in.at[me_p],
            device_id=there(0, j),
            device_id_type=MESH,
        )

    def send_best(g):
        for j in range(2):

            @pl.when((g == 0) & jnp.logical_not((me_p == 0) & (me_j == j)))
            def _():
                direct_copy(j).start()

        for k in range(finishers):
            j = lax.rem(me_j // 2 + k, finishers) * 2 + 1

            @pl.when((j != me_j) & jnp.logical_not((g == 0) & (j == 1)))
            def _():
                best_copy(g, j).start()

    width = best.shape[2]
    own_tokens = tokens // n_patches
    column = lax.broadcasted_iota(jnp.int32, (send.shape[1], width), 1)
    query = lax.broadcasted_iota(jnp.int32, (send.shape[1], width), 0)
    position = column // own_tokens
    named = position // (n_patches * nq) * nq + position % nq
    mean = jnp.where(named == query, 1.0 / tokens, 0.0)

    def score_copy(g, k):
        return pltpu.make_async_remote_copy(
            src_ref=send.at[g],
            dst_ref=arrived.at[me_p],
            send_sem=s_out,
            recv_sem=s_in.at[me_p],
            device_id=there(g, me_j - k),
            device_id_type=MESH,
        )

    def mean_of(total):
        return lax.dot_general(
            mean,
            total,
            (((1,), (1,)), ((), ())),
            precision=lax.Precision.HIGHEST,
            preferred_element_type=jnp.float32,
        )

    def finish(step):
        g = group(step)
        others = best_in.at[g, pl.ds(0, n_patches - 1)]
        pltpu.make_async_copy(others, others, b_in.at[g]).wait()
        total = best[g]
        for k in range(1, n_patches):
            total = jnp.maximum(total, best_in[g, lax.rem(me_j + k, n_patches)])
        send[g, :, :pairs] = mean_of(total)
        score_copy(g, 1).start()

        @pl.when(g == me_p)
        def _():
            arrived[me_p] = send[g]

        @pl.when(g != me_p)
        def _():
            score_copy(g, 0).start()

    def take(step):
        g = group(step)

        @pl.when(g == me_p)
        def _():
            some = q_all.at[g, pl.ds(0, n_patches - 1)]
            pltpu.make_async_copy(some, some, q_in.at[g]).wait()
            own_list.wait()

        @pl.when(g != me_p)
        def _():
            some = q_all.at[g]
            pltpu.make_async_copy(some, some, q_in.at[g]).wait()
            pltpu.make_async_copy(slots.at[g], slots.at[g], l_in.at[g]).wait()

        maxima(g)
        send_best(g)

    def maybe_finish(step):
        @pl.when(finisher & jnp.logical_not((me_j == 1) & (group(step) == 0)))
        def _():
            finish(step)

    gallery_copy.wait()
    last = n_pages - 1
    if n_pages <= 4:
        for step in range(n_pages):
            take(step)
            if step >= 2:
                maybe_finish(step - 2)
        for step in range(max(n_pages - 2, 0), n_pages):
            maybe_finish(step)
    else:

        @pl.loop(0, last)
        def _(step):
            take(step)
            maybe_finish(step)

        take(last)
        maybe_finish(last)

    def wait(units, sem):
        pltpu.make_async_copy(units, units, sem).wait()

    def drain_maxima():
        wait(q_all.at[pl.ds(0, n_pages - 1)], q_out)
        wait(q_all.at[0, pl.ds(0, n_patches - 1)], q_out)
        wait(lists.at[pl.ds(0, n_pages - 1)], l_out)

        def wait_best(full, last):
            if full > 0:
                wait(best_in.at[pl.ds(0, n_pages - 1), pl.ds(0, full)], b_out)
            if last > 0:
                wait(best_in.at[0, pl.ds(0, last)], b_out)

        @pl.when(jnp.logical_not(finisher))
        def _():
            wait_best(finishers, finishers - 1)

        @pl.when(me_j == 1)
        def _():
            wait_best(finishers - 1, finishers - 1)

        @pl.when(finisher & (me_j > 1))
        def _():
            wait_best(finishers - 1, finishers - 2)

        wait(best.at[0], d_out)

        @pl.when(jnp.logical_not(direct))
        def _():
            wait(best.at[0], d_out)

    def drain_scores():
        @pl.when(me_j == 1)
        def _():
            wait(send.at[pl.ds(0, n_pages - 1)], s_out)

            @pl.when(me_p > 0)
            def _():
                wait(send.at[pl.ds(0, n_pages - 2)], s_out)

            @pl.when(me_p == 0)
            def _():
                wait(send.at[pl.ds(0, n_pages - 1)], s_out)

        @pl.when(finisher & (me_j > 1))
        def _():
            wait(send.at[pl.ds(0, n_pages)], s_out)
            wait(send.at[pl.ds(0, n_pages - 1)], s_out)

    drain_maxima()
    cands = cand_ref.shape[1]
    spots = lax.broadcasted_iota(jnp.int32, (cands, pairs), 1)
    zeros = tuple(jnp.zeros((cands, pairs), jnp.float32) for _ in range(nq))

    def pick(h, scores, picked):
        found = []
        for q in range(nq):
            mine = key[q * cands : (q + 1) * cands]
            total = picked[q]
            for half in range(2):
                spot = (spots + (h * lanes + half * pairs)).astype(jnp.float32)
                line = scores[half * nq + q : half * nq + q + 1, :]
                total = total + jnp.where(mine == spot, line, 0.0)
            found.append(total)
        return tuple(found)

    def put(picked):
        for q in range(nq):
            out_ref[q : q + 1, :] = to_row(jnp.sum(picked[q], axis=1, keepdims=True))

    def over_others(step, picked):
        if n_pages <= 16:
            for k in range(n_pages - 1):
                picked = step(k, picked)
            return picked
        return lax.fori_loop(0, n_pages - 1, step, picked)

    @pl.when(direct)
    def _():
        key_rows = [to_row(key[q * cands : (q + 1) * cands]) for q in range(nq)]
        slot = lax.broadcasted_iota(jnp.int32, (pairs, cands), 0)
        lane_of = lax.broadcasted_iota(jnp.int32, (pairs, width), 1) // own_tokens
        kind = lane_of // (n_patches * nq) * nq + lane_of % nq

        def hits(h):
            return [
                (slot + (h * lanes + half * pairs)).astype(jnp.float32) == key_rows[q]
                for half in range(2)
                for q in range(nq)
            ]

        def add(hit, total, sums):
            sums = list(sums)
            for k in range(2 * nq):
                score = jnp.sum(jnp.where(kind == k, total, 0.0), axis=1, keepdims=True)
                sums[k % nq] = sums[k % nq] + jnp.where(hit[k], score, 0.0)
            return tuple(sums)

        sums = tuple(jnp.zeros((pairs, cands), jnp.float32) for _ in range(nq))
        wait(direct_in.at[0, pl.ds(0, n_patches - 1)], d_in.at[0])
        total = best[0]
        for k in range(1, n_patches):
            total = jnp.maximum(total, direct_in[0, lax.rem(me_j + k, n_patches)])
        sums = add(hits(0), total, sums)

        def later(k, sums):
            h = k + 1
            hit = hits(h)
            wait(direct_in.at[h], d_in.at[h])
            total = direct_in[h, 0]
            for j in range(1, n_patches):
                total = jnp.maximum(total, direct_in[h, j])
            return add(hit, total, sums)

        sums = over_others(later, sums)
        for q in range(nq):
            out_ref[q : q + 1, :] = jnp.sum(sums[q], axis=0, keepdims=True) * (1.0 / tokens)

    @pl.when(jnp.logical_not(direct))
    def _():
        def wait_scores(h):
            pltpu.make_async_copy(arrived.at[h], arrived.at[h], s_in.at[h]).wait()

        @pl.when(jnp.logical_not(finisher))
        def _():
            wait_scores(me_p)

        def scores_of(h):
            return arrived[h, :, :pairs]

        def later(k, picked):
            h = holder(n_pages - 2 - k)
            wait_scores(h)
            return pick(h, scores_of(h), picked)

        put(over_others(later, pick(me_p, scores_of(me_p), zeros)))

    drain_scores()


def body(queries, gallery, page_rows, candidates):
    nq, own_tokens, dim = queries.shape
    n_pages, n_patches = lax.axis_size("pages"), lax.axis_size("patches")
    most = 3 * nq * candidates.shape[1] // n_pages
    pairs = up(up(most, 2) // 2, 8)
    lanes = up(2 * pairs, 128)
    width = 2 * n_patches * nq * own_tokens
    vmem = pl.BlockSpec(memory_space=pltpu.VMEM)
    dma = pltpu.SemaphoreType.DMA
    return pl.pallas_call(
        functools.partial(kernel, (n_pages, n_patches, nq, own_tokens * n_patches)),
        out_shape=pltpu.VMEM(candidates.shape, jnp.float32),
        in_specs=[pl.BlockSpec(memory_space=pl.ANY)] * 4,
        out_specs=vmem,
        scratch_shapes=[
            pltpu.VMEM((nq * own_tokens, dim), jnp.bfloat16),
            pltpu.VMEM(page_rows.shape, jnp.int32),
            pltpu.VMEM(candidates.shape, jnp.int32),
            pltpu.VMEM((n_pages, n_patches, nq * own_tokens, dim), jnp.bfloat16),
            pltpu.VMEM(gallery.shape, jnp.bfloat16),
            pltpu.VMEM((n_pages, 1, lanes), jnp.int32),
            pltpu.SMEM((n_pages, 1, lanes), jnp.int32),
            pltpu.VMEM((n_pages, pairs, width), jnp.float32),
            pltpu.VMEM((n_pages, n_patches, pairs, width), jnp.float32),
            pltpu.VMEM((n_pages, n_patches, pairs, width), jnp.float32),
            pltpu.VMEM((n_pages, up(2 * nq, 8), lanes), jnp.float32),
            pltpu.VMEM((n_pages, up(2 * nq, 8), lanes), jnp.float32),
            dma,
            dma((3,)),
            dma,
            dma((n_pages,)),
            dma,
            dma,
            dma((n_pages,)),
            dma,
            dma((n_pages,)),
            dma,
            dma((n_pages,)),
            dma,
            dma((n_pages,)),
            pltpu.SemaphoreType.REGULAR((n_pages,)),
        ],
        compiler_params=pltpu.CompilerParams(collective_id=0, has_side_effects=True),
    )(
        queries.reshape(nq * own_tokens, dim),
        gallery,
        page_rows,
        candidates,
    )


def solution(mesh):
    in_specs = (
        P(("groups", "pages"), "patches", None),
        P(("groups", "pages"), "patches", None),
        P("groups"),
        P(("groups", "pages"), None),
    )
    out_specs = P(("groups", "pages"), None)
    return jax.shard_map(body, mesh=mesh, in_specs=in_specs, out_specs=out_specs, check_vma=False)
```

```python
import functools

import jax
import jax.numpy as jnp
from jax import lax
from jax.experimental import pallas as pl
from jax.experimental.pallas import tpu as pltpu
from jax.sharding import PartitionSpec as P

MESH = pl.DeviceIdType.MESH


def up(n, m):
    return -(-n // m) * m


def repeat(n, body):
    if n <= 16:
        for k in range(n):
            body(k)
    else:

        @pl.loop(0, n)
        def _(k):
            body(k)


def to_column(row):
    n = row.shape[1]
    eye = lax.broadcasted_iota(jnp.int32, (n, n), 0) == lax.broadcasted_iota(jnp.int32, (n, n), 1)
    return jnp.sum(jnp.where(eye, row, 0.0), axis=1, keepdims=True)


def to_row(column):
    n = column.shape[0]
    eye = lax.broadcasted_iota(jnp.int32, (n, n), 0) == lax.broadcasted_iota(jnp.int32, (n, n), 1)
    return jnp.sum(jnp.where(eye, column, 0.0), axis=0, keepdims=True)


def top_row(sims):
    rows, width = sims.shape
    chains = 4
    if rows % (8 * chains) == 0:
        sims = jnp.max(sims.reshape(rows // (8 * chains), chains, 8, width), axis=0)
        sims = jnp.maximum(jnp.maximum(sims[0], sims[1]), jnp.maximum(sims[2], sims[3]))
    return jnp.max(sims, axis=0, keepdims=True)


def kernel(
    dims,
    q_hbm,
    g_ref,
    rows_hbm,
    cand_hbm,
    out_ref,
    q_ref,
    rows_ref,
    cand_ref,
    q_all,
    g_buf,
    lists,
    slots,
    best,
    best_in,
    direct_in,
    send,
    arrived,
    g_sem,
    a_sem,
    q_out,
    q_in,
    l_own,
    l_out,
    l_in,
    b_out,
    b_in,
    s_out,
    s_in,
    d_out,
    d_in,
    ready,
):
    n_pages, n_patches, nq, tokens = dims
    devices = n_pages * n_patches
    page_count = g_ref.shape[0]
    pairs = best.shape[1]
    lanes = lists.shape[2]
    me_g = lax.axis_index("groups")
    me_p = lax.axis_index("pages")
    me_j = lax.axis_index("patches")
    finisher = lax.rem(me_j, 2) == 1
    finishers = n_patches // 2
    direct = (me_p == 0) & (me_j < 2)

    def there(p, j):
        return (me_g, p, j)

    def holder(k):
        k = jnp.int32(k)
        below = me_p
        above = n_pages - 1 - me_p
        both = 2 * jnp.minimum(below, above)
        longest = jnp.maximum(below, above)
        single = longest - both // 2
        first = jnp.where(below > above, k, n_pages - 1 - k)
        rest = k - single
        alternating = jnp.where(
            lax.rem(rest, 2) == 0, both // 2 - rest // 2, -(both // 2 - rest // 2)
        )
        return jnp.where(k < single, first, me_p + alternating)

    def group(step):
        step = jnp.int32(step)
        low = jnp.where(step <= me_p, step - 1, step)
        high = jnp.where(step < me_p, me_p - 1 - step, step)
        high = jnp.where(step == me_p, me_p - 1, high)
        return jnp.where(step == 0, me_p, jnp.where(me_p > 2, high, low))

    barrier = pltpu.get_barrier_semaphore()

    def greet(p, j):
        pl.semaphore_signal(barrier, inc=1, device_id=there(p, j), device_id_type=MESH)

    def across(p, first, act):
        for k in range(first, n_patches):
            act(p, lax.rem(me_j + k, n_patches))

    def above(act):
        def one(k):
            @pl.when(n_pages - 1 - k > me_p)
            def _():
                act(n_pages - 1 - k)

        repeat(n_pages - 1, one)

    def below(act):
        def one(k):
            @pl.when(k < me_p)
            def _():
                act(k)

        repeat(n_pages - 1, one)

    across(me_p, 1, greet)
    above(lambda p: across(p, 0, greet))
    small = [
        pltpu.make_async_copy(source, target, a_sem.at[k])
        for k, (source, target) in enumerate(
            ((q_hbm, q_ref), (cand_hbm, cand_ref), (rows_hbm, rows_ref))
        )
    ]
    for copy in small:
        copy.start()
    gallery_copy = pltpu.make_async_copy(g_ref, g_buf, g_sem)
    gallery_copy.start()
    send[...] = jnp.zeros_like(send)
    pl.semaphore_wait(barrier, n_patches - 1 + n_patches * me_p)

    def announce(p):
        for k in range(2):
            pl.semaphore_signal(
                ready.at[me_p], inc=1, device_id=there(p, me_j - k), device_id_type=MESH
            )

    @pl.when(finisher)
    def _():
        below(announce)

    for copy in small:
        copy.wait()

    q_all[me_p, me_j] = q_ref[...]
    def send_queries(p, j):
        pltpu.make_async_remote_copy(
            src_ref=q_ref,
            dst_ref=q_all.at[me_p, me_j],
            send_sem=q_out,
            recv_sem=q_in.at[me_p],
            device_id=there(p, j),
            device_id_type=MESH,
        ).start()

    across(me_p, 1, send_queries)
    below(lambda p: across(p, 0, send_queries))

    page_rows = rows_ref[...].astype(jnp.float32).reshape(1, -1)
    columns = []
    for q in range(nq):
        wanted = to_column(cand_ref[q : q + 1, :].astype(jnp.float32))
        ids = lax.broadcasted_iota(jnp.int32, (wanted.shape[0], page_rows.shape[1]), 1)
        hit = ids.astype(jnp.float32) == wanted
        columns.append(jnp.sum(jnp.where(hit, page_rows, 0.0), axis=1, keepdims=True))
    row = jnp.concatenate(columns, axis=0)
    held_by = jnp.zeros_like(row)
    for h in range(1, n_pages):
        held_by = held_by + jnp.where(row >= float(h * page_count), 1.0, 0.0)
    local = row - held_by * float(page_count)
    n = row.shape[0]
    earlier = lax.broadcasted_iota(jnp.int32, (n, n), 1) < lax.broadcasted_iota(jnp.int32, (n, n), 0)
    same = to_row(held_by) == held_by
    place = jnp.sum(jnp.where(earlier & same, 1.0, 0.0), axis=1, keepdims=True)
    key = held_by * float(lanes) + place
    lane = lax.broadcasted_iota(jnp.int32, (n, lanes), 1)

    def make_list(h):
        chosen = key == (lane + h * lanes).astype(jnp.float32)
        found = jnp.sum(jnp.where(chosen, local, 0.0), axis=0, keepdims=True).astype(jnp.int32)
        lists[h] = jnp.clip(found, 0, page_count - 1)

    repeat(n_pages, make_list)
    own_list = pltpu.make_async_copy(lists.at[me_p], slots.at[me_p], l_own)
    own_list.start()

    def send_list(p):
        pltpu.make_async_remote_copy(
            src_ref=lists.at[p],
            dst_ref=slots.at[me_p],
            send_sem=l_out,
            recv_sem=l_in.at[me_p],
            device_id=there(p, me_j),
            device_id_type=MESH,
        ).start()

    below(send_list)

    def send_above(k):
        @pl.when(k + 1 > me_p)
        def _():
            pl.semaphore_wait(ready.at[k + 1], 1)
            for spread in reversed(range(n_patches)):
                send_queries(k + 1, lax.rem(me_j + spread, n_patches))
            send_list(k + 1)

    repeat(n_pages - 1, send_above)

    def maxima(g):
        rows = q_all[g].reshape(n_patches * q_all.shape[2], q_all.shape[3])
        none = jnp.zeros_like(rows)
        weights = jnp.concatenate(
            [jnp.concatenate([rows, none], axis=1), jnp.concatenate([none, rows], axis=1)], axis=0
        )
        for k in range(pairs):
            pair = jnp.concatenate([g_buf[slots[g, 0, k]], g_buf[slots[g, 0, pairs + k]]], axis=1)
            sims = lax.dot_general(
                pair, weights, (((1,), (1,)), ((), ())), preferred_element_type=jnp.float32
            )
            best[g, k : k + 1, :] = top_row(sims)

    def best_copy(g, j):
        return pltpu.make_async_remote_copy(
            src_ref=best.at[g],
            dst_ref=best_in.at[g, me_j],
            send_sem=b_out,
            recv_sem=b_in.at[g],
            device_id=there(me_p, j),
            device_id_type=MESH,
        )

    def direct_copy(j):
        return pltpu.make_async_remote_copy(
            src_ref=best.at[0],
            dst_ref=direct_in.at[me_p, me_j],
            send_sem=d_out,
            recv_sem=d_in.at[me_p],
            device_id=there(0, j),
            device_id_type=MESH,
        )

    def send_best(g):
        for j in range(2):

            @pl.when((g == 0) & jnp.logical_not((me_p == 0) & (me_j == j)))
            def _():
                direct_copy(j).start()

        for k in range(finishers):
            j = lax.rem(me_j // 2 + k, finishers) * 2 + 1

            @pl.when((j != me_j) & jnp.logical_not((g == 0) & (j == 1)))
            def _():
                best_copy(g, j).start()

    width = best.shape[2]
    own_tokens = tokens // n_patches
    column = lax.broadcasted_iota(jnp.int32, (send.shape[1], width), 1)
    query = lax.broadcasted_iota(jnp.int32, (send.shape[1], width), 0)
    position = column // own_tokens
    named = position // (n_patches * nq) * nq + position % nq
    mean = jnp.where(named == query, 1.0 / tokens, 0.0)

    def score_copy(g, k):
        return pltpu.make_async_remote_copy(
            src_ref=send.at[g],
            dst_ref=arrived.at[me_p],
            send_sem=s_out,
            recv_sem=s_in.at[me_p],
            device_id=there(g, me_j - k),
            device_id_type=MESH,
        )

    def mean_of(total):
        return lax.dot_general(
            mean,
            total,
            (((1,), (1,)), ((), ())),
            precision=lax.Precision.HIGHEST,
            preferred_element_type=jnp.float32,
        )

    def finish(step):
        g = group(step)
        others = best_in.at[g, pl.ds(0, n_patches - 1)]
        pltpu.make_async_copy(others, others, b_in.at[g]).wait()
        total = best[g]
        for k in range(1, n_patches):
            total = jnp.maximum(total, best_in[g, lax.rem(me_j + k, n_patches)])
        send[g, :, :pairs] = mean_of(total)
        score_copy(g, 1).start()

        @pl.when(g == me_p)
        def _():
            arrived[me_p] = send[g]

        @pl.when(g != me_p)
        def _():
            score_copy(g, 0).start()

    def take(step):
        g = group(step)

        @pl.when(g == me_p)
        def _():
            some = q_all.at[g, pl.ds(0, n_patches - 1)]
            pltpu.make_async_copy(some, some, q_in.at[g]).wait()
            own_list.wait()

        @pl.when(g != me_p)
        def _():
            some = q_all.at[g]
            pltpu.make_async_copy(some, some, q_in.at[g]).wait()
            pltpu.make_async_copy(slots.at[g], slots.at[g], l_in.at[g]).wait()

        maxima(g)
        send_best(g)

    def maybe_finish(step):
        @pl.when(finisher & jnp.logical_not((me_j == 1) & (group(step) == 0)))
        def _():
            finish(step)

    gallery_copy.wait()
    last = n_pages - 1
    if n_pages <= 4:
        for step in range(n_pages):
            take(step)
            if step >= 2:
                maybe_finish(step - 2)
        for step in range(max(n_pages - 2, 0), n_pages):
            maybe_finish(step)
    else:

        @pl.loop(0, last)
        def _(step):
            take(step)
            maybe_finish(step)

        take(last)
        maybe_finish(last)

    def wait(units, sem):
        pltpu.make_async_copy(units, units, sem).wait()

    def drain_maxima():
        wait(q_all.at[pl.ds(0, n_pages - 1)], q_out)
        wait(q_all.at[0, pl.ds(0, n_patches - 1)], q_out)
        wait(lists.at[pl.ds(0, n_pages - 1)], l_out)

        def wait_best(full, last):
            if full > 0:
                wait(best_in.at[pl.ds(0, n_pages - 1), pl.ds(0, full)], b_out)
            if last > 0:
                wait(best_in.at[0, pl.ds(0, last)], b_out)

        @pl.when(jnp.logical_not(finisher))
        def _():
            wait_best(finishers, finishers - 1)

        @pl.when(me_j == 1)
        def _():
            wait_best(finishers - 1, finishers - 1)

        @pl.when(finisher & (me_j > 1))
        def _():
            wait_best(finishers - 1, finishers - 2)

        wait(best.at[0], d_out)

        @pl.when(jnp.logical_not(direct))
        def _():
            wait(best.at[0], d_out)

    def drain_scores():
        @pl.when(me_j == 1)
        def _():
            wait(send.at[pl.ds(0, n_pages - 1)], s_out)

            @pl.when(me_p > 0)
            def _():
                wait(send.at[pl.ds(0, n_pages - 2)], s_out)

            @pl.when(me_p == 0)
            def _():
                wait(send.at[pl.ds(0, n_pages - 1)], s_out)

        @pl.when(finisher & (me_j > 1))
        def _():
            wait(send.at[pl.ds(0, n_pages)], s_out)
            wait(send.at[pl.ds(0, n_pages - 1)], s_out)

    drain_maxima()
    cands = cand_ref.shape[1]
    spots = lax.broadcasted_iota(jnp.int32, (cands, pairs), 1)
    zeros = tuple(jnp.zeros((cands, pairs), jnp.float32) for _ in range(nq))

    def pick(h, scores, picked):
        found = []
        for q in range(nq):
            mine = key[q * cands : (q + 1) * cands]
            total = picked[q]
            for half in range(2):
                spot = (spots + (h * lanes + half * pairs)).astype(jnp.float32)
                line = scores[half * nq + q : half * nq + q + 1, :]
                total = total + jnp.where(mine == spot, line, 0.0)
            found.append(total)
        return tuple(found)

    def put(picked):
        for q in range(nq):
            out_ref[q : q + 1, :] = to_row(jnp.sum(picked[q], axis=1, keepdims=True))

    def over_others(step, picked):
        if n_pages <= 16:
            for k in range(n_pages - 1):
                picked = step(k, picked)
            return picked
        return lax.fori_loop(0, n_pages - 1, step, picked)

    @pl.when(jnp.logical_not(direct))
    def _():
        def wait_scores(h):
            pltpu.make_async_copy(arrived.at[h], arrived.at[h], s_in.at[h]).wait()

        @pl.when(jnp.logical_not(finisher))
        def _():
            wait_scores(me_p)

        def scores_of(h):
            return arrived[h, :, :pairs]

        def later(k, picked):
            h = holder(n_pages - 2 - k)
            wait_scores(h)
            return pick(h, scores_of(h), picked)

        put(over_others(later, pick(me_p, scores_of(me_p), zeros)))

    @pl.when(direct)
    def _():
        key_rows = [to_row(key[q * cands : (q + 1) * cands]) for q in range(nq)]
        slot = lax.broadcasted_iota(jnp.int32, (pairs, cands), 0)
        lane_of = lax.broadcasted_iota(jnp.int32, (pairs, width), 1) // own_tokens
        kind = lane_of // (n_patches * nq) * nq + lane_of % nq

        def hits(h):
            return [
                (slot + (h * lanes + half * pairs)).astype(jnp.float32) == key_rows[q]
                for half in range(2)
                for q in range(nq)
            ]

        def add(hit, total, sums):
            sums = list(sums)
            for k in range(2 * nq):
                score = jnp.sum(jnp.where(kind == k, total, 0.0), axis=1, keepdims=True)
                sums[k % nq] = sums[k % nq] + jnp.where(hit[k], score, 0.0)
            return tuple(sums)

        sums = tuple(jnp.zeros((pairs, cands), jnp.float32) for _ in range(nq))
        wait(direct_in.at[0, pl.ds(0, n_patches - 1)], d_in.at[0])
        total = best[0]
        for k in range(1, n_patches):
            total = jnp.maximum(total, direct_in[0, lax.rem(me_j + k, n_patches)])
        sums = add(hits(0), total, sums)

        def later(k, sums):
            h = k + 1
            hit = hits(h)
            wait(direct_in.at[h], d_in.at[h])
            total = direct_in[h, 0]
            for j in range(1, n_patches):
                total = jnp.maximum(total, direct_in[h, j])
            return add(hit, total, sums)

        sums = over_others(later, sums)
        for q in range(nq):
            out_ref[q : q + 1, :] = jnp.sum(sums[q], axis=0, keepdims=True) * (1.0 / tokens)

    drain_scores()


def body(queries, gallery, page_rows, candidates):
    nq, own_tokens, dim = queries.shape
    n_pages, n_patches = lax.axis_size("pages"), lax.axis_size("patches")
    most = 3 * nq * candidates.shape[1] // n_pages
    pairs = up(up(most, 2) // 2, 8)
    lanes = up(2 * pairs, 128)
    width = 2 * n_patches * nq * own_tokens
    vmem = pl.BlockSpec(memory_space=pltpu.VMEM)
    dma = pltpu.SemaphoreType.DMA
    return pl.pallas_call(
        functools.partial(kernel, (n_pages, n_patches, nq, own_tokens * n_patches)),
        out_shape=pltpu.VMEM(candidates.shape, jnp.float32),
        in_specs=[pl.BlockSpec(memory_space=pl.ANY)] * 4,
        out_specs=vmem,
        scratch_shapes=[
            pltpu.VMEM((nq * own_tokens, dim), jnp.bfloat16),
            pltpu.VMEM(page_rows.shape, jnp.int32),
            pltpu.VMEM(candidates.shape, jnp.int32),
            pltpu.VMEM((n_pages, n_patches, nq * own_tokens, dim), jnp.bfloat16),
            pltpu.VMEM(gallery.shape, jnp.bfloat16),
            pltpu.VMEM((n_pages, 1, lanes), jnp.int32),
            pltpu.SMEM((n_pages, 1, lanes), jnp.int32),
            pltpu.VMEM((n_pages, pairs, width), jnp.float32),
            pltpu.VMEM((n_pages, n_patches, pairs, width), jnp.float32),
            pltpu.VMEM((n_pages, n_patches, pairs, width), jnp.float32),
            pltpu.VMEM((n_pages, up(2 * nq, 8), lanes), jnp.float32),
            pltpu.VMEM((n_pages, up(2 * nq, 8), lanes), jnp.float32),
            dma,
            dma((3,)),
            dma,
            dma((n_pages,)),
            dma,
            dma,
            dma((n_pages,)),
            dma,
            dma((n_pages,)),
            dma,
            dma((n_pages,)),
            dma,
            dma((n_pages,)),
            pltpu.SemaphoreType.REGULAR((n_pages,)),
        ],
        compiler_params=pltpu.CompilerParams(collective_id=0, has_side_effects=True),
    )(
        queries.reshape(nq * own_tokens, dim),
        gallery,
        page_rows,
        candidates,
    )


def solution(mesh):
    in_specs = (
        P(("groups", "pages"), "patches", None),
        P(("groups", "pages"), "patches", None),
        P("groups"),
        P(("groups", "pages"), None),
    )
    out_specs = P(("groups", "pages"), None)
    return jax.shard_map(body, mesh=mesh, in_specs=in_specs, out_specs=out_specs, check_vma=False)
```

```python
import functools

import jax
import jax.numpy as jnp
from jax import lax
from jax.experimental import pallas as pl
from jax.experimental.pallas import tpu as pltpu
from jax.sharding import PartitionSpec as P

MESH = pl.DeviceIdType.MESH


def up(n, m):
    return -(-n // m) * m


def repeat(n, body):
    if n <= 16:
        for k in range(n):
            body(k)
    else:

        @pl.loop(0, n)
        def _(k):
            body(k)


def to_column(row):
    n = row.shape[1]
    eye = lax.broadcasted_iota(jnp.int32, (n, n), 0) == lax.broadcasted_iota(jnp.int32, (n, n), 1)
    return jnp.sum(jnp.where(eye, row, 0.0), axis=1, keepdims=True)


def to_row(column):
    n = column.shape[0]
    eye = lax.broadcasted_iota(jnp.int32, (n, n), 0) == lax.broadcasted_iota(jnp.int32, (n, n), 1)
    return jnp.sum(jnp.where(eye, column, 0.0), axis=0, keepdims=True)


def top_row(sims):
    rows, width = sims.shape
    chains = 4
    if rows % (8 * chains) == 0:
        sims = jnp.max(sims.reshape(rows // (8 * chains), chains, 8, width), axis=0)
        sims = jnp.maximum(jnp.maximum(sims[0], sims[1]), jnp.maximum(sims[2], sims[3]))
    return jnp.max(sims, axis=0, keepdims=True)


def kernel(
    dims,
    q_hbm,
    g_ref,
    rows_hbm,
    cand_hbm,
    out_ref,
    q_ref,
    rows_ref,
    cand_ref,
    q_all,
    g_buf,
    lists,
    slots,
    best,
    best_in,
    direct_in,
    send,
    arrived,
    g_sem,
    a_sem,
    q_out,
    q_in,
    l_own,
    l_out,
    l_in,
    b_out,
    b_in,
    s_out,
    s_in,
    d_out,
    d_in,
    ready,
):
    n_pages, n_patches, nq, tokens = dims
    devices = n_pages * n_patches
    page_count = g_ref.shape[0]
    packed = best.shape[1]
    pairs = packed * nq
    lanes = lists.shape[2]
    own_tokens = tokens // n_patches
    me_g = lax.axis_index("groups")
    me_p = lax.axis_index("pages")
    me_j = lax.axis_index("patches")
    finisher = lax.rem(me_j, 2) == 1
    finishers = n_patches // 2
    direct = (me_p == 0) & (me_j < 2)

    def there(p, j):
        return (me_g, p, j)

    def holder(k):
        k = jnp.int32(k)
        below = me_p
        above = n_pages - 1 - me_p
        both = 2 * jnp.minimum(below, above)
        longest = jnp.maximum(below, above)
        single = longest - both // 2
        first = jnp.where(below > above, k, n_pages - 1 - k)
        rest = k - single
        alternating = jnp.where(
            lax.rem(rest, 2) == 0, both // 2 - rest // 2, -(both // 2 - rest // 2)
        )
        return jnp.where(k < single, first, me_p + alternating)

    def group(step):
        step = jnp.int32(step)
        low = jnp.where(step <= me_p, step - 1, step)
        high = jnp.where(step < me_p, me_p - 1 - step, step)
        high = jnp.where(step == me_p, me_p - 1, high)
        return jnp.where(step == 0, me_p, jnp.where(me_p > 2, high, low))

    barrier = pltpu.get_barrier_semaphore()

    def greet(p, j):
        pl.semaphore_signal(barrier, inc=1, device_id=there(p, j), device_id_type=MESH)

    def across(p, first, act):
        for k in range(first, n_patches):
            act(p, lax.rem(me_j + k, n_patches))

    def above(act):
        def one(k):
            @pl.when(n_pages - 1 - k > me_p)
            def _():
                act(n_pages - 1 - k)

        repeat(n_pages - 1, one)

    def below(act):
        def one(k):
            @pl.when(k < me_p)
            def _():
                act(k)

        repeat(n_pages - 1, one)

    across(me_p, 1, greet)
    above(lambda p: across(p, 0, greet))
    small = [
        pltpu.make_async_copy(source, target, a_sem.at[k])
        for k, (source, target) in enumerate(
            ((q_hbm, q_ref), (cand_hbm, cand_ref), (rows_hbm, rows_ref))
        )
    ]
    for copy in small:
        copy.start()
    gallery_copy = pltpu.make_async_copy(g_ref, g_buf, g_sem)
    gallery_copy.start()
    send[...] = jnp.zeros_like(send)
    pl.semaphore_wait(barrier, n_patches - 1 + n_patches * me_p)

    def announce(p):
        for k in range(2):
            pl.semaphore_signal(
                ready.at[me_p], inc=1, device_id=there(p, me_j - k), device_id_type=MESH
            )

    @pl.when(finisher)
    def _():
        below(announce)

    for copy in small:
        copy.wait()

    q_all[me_p, me_j] = q_ref[...]
    def send_queries(p, j):
        pltpu.make_async_remote_copy(
            src_ref=q_ref,
            dst_ref=q_all.at[me_p, me_j],
            send_sem=q_out,
            recv_sem=q_in.at[me_p],
            device_id=there(p, j),
            device_id_type=MESH,
        ).start()

    across(me_p, 1, send_queries)
    below(lambda p: across(p, 0, send_queries))

    page_rows = rows_ref[...].astype(jnp.float32).reshape(1, -1)
    columns = []
    for q in range(nq):
        wanted = to_column(cand_ref[q : q + 1, :].astype(jnp.float32))
        ids = lax.broadcasted_iota(jnp.int32, (wanted.shape[0], page_rows.shape[1]), 1)
        hit = ids.astype(jnp.float32) == wanted
        columns.append(jnp.sum(jnp.where(hit, page_rows, 0.0), axis=1, keepdims=True))
    row = jnp.concatenate(columns, axis=0)
    held_by = jnp.zeros_like(row)
    for h in range(1, n_pages):
        held_by = held_by + jnp.where(row >= float(h * page_count), 1.0, 0.0)
    local = row - held_by * float(page_count)
    n = row.shape[0]
    asker = jnp.concatenate(
        [jnp.full_like(columns[q], float(q)) for q in range(nq)], axis=0
    )
    entry = local * float(nq) + asker
    earlier = lax.broadcasted_iota(jnp.int32, (n, n), 1) < lax.broadcasted_iota(jnp.int32, (n, n), 0)
    same = to_row(held_by) == held_by
    place = jnp.sum(jnp.where(earlier & same, 1.0, 0.0), axis=1, keepdims=True)
    key = held_by * float(lanes) + place
    lane = lax.broadcasted_iota(jnp.int32, (n, lanes), 1)

    def make_list(h):
        chosen = key == (lane + h * lanes).astype(jnp.float32)
        found = jnp.sum(jnp.where(chosen, entry, 0.0), axis=0, keepdims=True).astype(jnp.int32)
        lists[h] = jnp.clip(found, 0, page_count * nq - 1)

    repeat(n_pages, make_list)
    own_list = pltpu.make_async_copy(lists.at[me_p], slots.at[me_p], l_own)
    own_list.start()

    def send_list(p):
        pltpu.make_async_remote_copy(
            src_ref=lists.at[p],
            dst_ref=slots.at[me_p],
            send_sem=l_out,
            recv_sem=l_in.at[me_p],
            device_id=there(p, me_j),
            device_id_type=MESH,
        ).start()

    below(send_list)

    def send_above(k):
        @pl.when(k + 1 > me_p)
        def _():
            pl.semaphore_wait(ready.at[k + 1], 1)
            for spread in reversed(range(n_patches)):
                send_queries(k + 1, lax.rem(me_j + spread, n_patches))
            send_list(k + 1)

    repeat(n_pages - 1, send_above)

    def maxima(g):
        rows = q_all[g].reshape(n_patches * q_all.shape[2], q_all.shape[3])
        none = jnp.zeros_like(rows)
        weights = jnp.concatenate(
            [jnp.concatenate([rows, none], axis=1), jnp.concatenate([none, rows], axis=1)], axis=0
        )
        lanes_of = lax.broadcasted_iota(jnp.int32, (1, best.shape[2]), 1)
        place_of = lanes_of // own_tokens % nq
        for r in range(packed):
            together = None
            for i in range(nq):
                k = i * packed + r
                ids = [slots[g, 0, k], slots[g, 0, pairs + k]]
                pair = jnp.concatenate([g_buf[lax.div(v, nq)] for v in ids], axis=1)
                sims = lax.dot_general(
                    pair, weights, (((1,), (1,)), ((), ())), preferred_element_type=jnp.float32
                )
                tops = top_row(sims)
                askers = [lax.rem(v, nq) for v in ids]
                asked = jnp.where(lanes_of < best.shape[2] // 2, askers[0], askers[1])
                here = tops
                for q in range(nq):
                    if q != i:
                        shift = (i - q) * own_tokens % best.shape[2]
                        here = jnp.where(asked == q, pltpu.roll(tops, shift, 1), here)
                together = here if i == 0 else jnp.where(place_of == i, here, together)
            best[g, r : r + 1, :] = together

    def best_copy(g, j):
        return pltpu.make_async_remote_copy(
            src_ref=best.at[g],
            dst_ref=best_in.at[g, me_j],
            send_sem=b_out,
            recv_sem=b_in.at[g],
            device_id=there(me_p, j),
            device_id_type=MESH,
        )

    def direct_copy(j):
        return pltpu.make_async_remote_copy(
            src_ref=best.at[0],
            dst_ref=direct_in.at[me_p, me_j],
            send_sem=d_out,
            recv_sem=d_in.at[me_p],
            device_id=there(0, j),
            device_id_type=MESH,
        )

    def send_best(g):
        for j in range(2):

            @pl.when((g == 0) & jnp.logical_not((me_p == 0) & (me_j == j)))
            def _():
                direct_copy(j).start()

        for k in range(finishers):
            j = lax.rem(me_j // 2 + k, finishers) * 2 + 1

            @pl.when((j != me_j) & jnp.logical_not((g == 0) & (j == 1)))
            def _():
                best_copy(g, j).start()

    width = best.shape[2]
    column = lax.broadcasted_iota(jnp.int32, (send.shape[1], width), 1)
    query = lax.broadcasted_iota(jnp.int32, (send.shape[1], width), 0)
    position = column // own_tokens
    named = position // (n_patches * nq) * nq + position % nq
    mean = jnp.where(named == query, 1.0 / tokens, 0.0)

    def score_copy(g, k):
        return pltpu.make_async_remote_copy(
            src_ref=send.at[g],
            dst_ref=arrived.at[me_p],
            send_sem=s_out,
            recv_sem=s_in.at[me_p],
            device_id=there(g, me_j - k),
            device_id_type=MESH,
        )

    def mean_of(total):
        return lax.dot_general(
            mean,
            total,
            (((1,), (1,)), ((), ())),
            precision=lax.Precision.HIGHEST,
            preferred_element_type=jnp.float32,
        )

    def finish(step):
        g = group(step)
        others = best_in.at[g, pl.ds(0, n_patches - 1)]
        pltpu.make_async_copy(others, others, b_in.at[g]).wait()
        total = best[g]
        for k in range(1, n_patches):
            total = jnp.maximum(total, best_in[g, lax.rem(me_j + k, n_patches)])
        send[g, :, :packed] = mean_of(total)
        score_copy(g, 1).start()

        @pl.when(g == me_p)
        def _():
            arrived[me_p] = send[g]

        @pl.when(g != me_p)
        def _():
            score_copy(g, 0).start()

    def take(step):
        g = group(step)

        @pl.when(g == me_p)
        def _():
            some = q_all.at[g, pl.ds(0, n_patches - 1)]
            pltpu.make_async_copy(some, some, q_in.at[g]).wait()
            own_list.wait()

        @pl.when(g != me_p)
        def _():
            some = q_all.at[g]
            pltpu.make_async_copy(some, some, q_in.at[g]).wait()
            pltpu.make_async_copy(slots.at[g], slots.at[g], l_in.at[g]).wait()

        maxima(g)
        send_best(g)

    def maybe_finish(step):
        @pl.when(finisher & jnp.logical_not((me_j == 1) & (group(step) == 0)))
        def _():
            finish(step)

    gallery_copy.wait()
    last = n_pages - 1
    if n_pages <= 4:
        for step in range(n_pages):
            take(step)
            if step >= 2:
                maybe_finish(step - 2)
        for step in range(max(n_pages - 2, 0), n_pages):
            maybe_finish(step)
    else:

        @pl.loop(0, last)
        def _(step):
            take(step)
            maybe_finish(step)

        take(last)
        maybe_finish(last)

    def wait(units, sem):
        pltpu.make_async_copy(units, units, sem).wait()

    def drain_maxima():
        wait(q_all.at[pl.ds(0, n_pages - 1)], q_out)
        wait(q_all.at[0, pl.ds(0, n_patches - 1)], q_out)
        wait(lists.at[pl.ds(0, n_pages - 1)], l_out)

        def wait_best(full, last):
            if full > 0:
                wait(best_in.at[pl.ds(0, n_pages - 1), pl.ds(0, full)], b_out)
            if last > 0:
                wait(best_in.at[0, pl.ds(0, last)], b_out)

        @pl.when(jnp.logical_not(finisher))
        def _():
            wait_best(finishers, finishers - 1)

        @pl.when(me_j == 1)
        def _():
            wait_best(finishers - 1, finishers - 1)

        @pl.when(finisher & (me_j > 1))
        def _():
            wait_best(finishers - 1, finishers - 2)

        wait(best.at[0], d_out)

        @pl.when(jnp.logical_not(direct))
        def _():
            wait(best.at[0], d_out)

    def drain_scores():
        @pl.when(me_j == 1)
        def _():
            wait(send.at[pl.ds(0, n_pages - 1)], s_out)

            @pl.when(me_p > 0)
            def _():
                wait(send.at[pl.ds(0, n_pages - 2)], s_out)

            @pl.when(me_p == 0)
            def _():
                wait(send.at[pl.ds(0, n_pages - 1)], s_out)

        @pl.when(finisher & (me_j > 1))
        def _():
            wait(send.at[pl.ds(0, n_pages)], s_out)
            wait(send.at[pl.ds(0, n_pages - 1)], s_out)

    drain_maxima()
    cands = cand_ref.shape[1]
    spots = lax.broadcasted_iota(jnp.int32, (cands, packed), 1)
    zeros = tuple(jnp.zeros((cands, packed), jnp.float32) for _ in range(nq))

    def pick(h, scores, picked):
        found = []
        for q in range(nq):
            mine = key[q * cands : (q + 1) * cands]
            total = picked[q]
            for kind in range(2 * nq):
                spot = (spots + (h * lanes + kind * packed)).astype(jnp.float32)
                total = total + jnp.where(mine == spot, scores[kind : kind + 1, :], 0.0)
            found.append(total)
        return tuple(found)

    def put(picked):
        for q in range(nq):
            out_ref[q : q + 1, :] = to_row(jnp.sum(picked[q], axis=1, keepdims=True))

    def over_others(step, picked):
        if n_pages <= 16:
            for k in range(n_pages - 1):
                picked = step(k, picked)
            return picked
        return lax.fori_loop(0, n_pages - 1, step, picked)

    @pl.when(jnp.logical_not(direct))
    def _():
        def wait_scores(h):
            pltpu.make_async_copy(arrived.at[h], arrived.at[h], s_in.at[h]).wait()

        @pl.when(jnp.logical_not(finisher))
        def _():
            wait_scores(me_p)

        def scores_of(h):
            return arrived[h, :, :packed]

        def later(k, picked):
            h = holder(n_pages - 2 - k)
            wait_scores(h)
            return pick(h, scores_of(h), picked)

        put(over_others(later, pick(me_p, scores_of(me_p), zeros)))

    @pl.when(direct)
    def _():
        key_rows = [to_row(key[q * cands : (q + 1) * cands]) for q in range(nq)]
        slot = lax.broadcasted_iota(jnp.int32, (packed, cands), 0)
        lane_of = lax.broadcasted_iota(jnp.int32, (packed, width), 1) // own_tokens
        kind_of = lane_of // (n_patches * nq) * nq + lane_of % nq

        def hits(h):
            spots = [
                (slot + (h * lanes + kind * packed)).astype(jnp.float32) for kind in range(2 * nq)
            ]
            return [[spot == key_row for key_row in key_rows] for spot in spots]

        def add(hit, total, sums):
            sums = list(sums)
            for kind in range(2 * nq):
                score = jnp.sum(jnp.where(kind_of == kind, total, 0.0), axis=1, keepdims=True)
                for q in range(nq):
                    sums[q] = sums[q] + jnp.where(hit[kind][q], score, 0.0)
            return tuple(sums)

        sums = tuple(jnp.zeros((packed, cands), jnp.float32) for _ in range(nq))
        wait(direct_in.at[0, pl.ds(0, n_patches - 1)], d_in.at[0])
        total = best[0]
        for k in range(1, n_patches):
            total = jnp.maximum(total, direct_in[0, lax.rem(me_j + k, n_patches)])
        sums = add(hits(0), total, sums)

        def later(k, sums):
            h = k + 1
            hit = hits(h)
            wait(direct_in.at[h], d_in.at[h])
            total = direct_in[h, 0]
            for j in range(1, n_patches):
                total = jnp.maximum(total, direct_in[h, j])
            return add(hit, total, sums)

        sums = over_others(later, sums)
        for q in range(nq):
            out_ref[q : q + 1, :] = jnp.sum(sums[q], axis=0, keepdims=True) * (1.0 / tokens)

    drain_scores()


def body(queries, gallery, page_rows, candidates):
    nq, own_tokens, dim = queries.shape
    n_pages, n_patches = lax.axis_size("pages"), lax.axis_size("patches")
    most = 3 * nq * candidates.shape[1] // n_pages
    packed = -(-most // (2 * nq))
    lanes = up(2 * nq * packed, 128)
    width = 2 * n_patches * nq * own_tokens
    vmem = pl.BlockSpec(memory_space=pltpu.VMEM)
    dma = pltpu.SemaphoreType.DMA
    return pl.pallas_call(
        functools.partial(kernel, (n_pages, n_patches, nq, own_tokens * n_patches)),
        out_shape=pltpu.VMEM(candidates.shape, jnp.float32),
        in_specs=[pl.BlockSpec(memory_space=pl.ANY)] * 4,
        out_specs=vmem,
        scratch_shapes=[
            pltpu.VMEM((nq * own_tokens, dim), jnp.bfloat16),
            pltpu.VMEM(page_rows.shape, jnp.int32),
            pltpu.VMEM(candidates.shape, jnp.int32),
            pltpu.VMEM((n_pages, n_patches, nq * own_tokens, dim), jnp.bfloat16),
            pltpu.VMEM(gallery.shape, jnp.bfloat16),
            pltpu.VMEM((n_pages, 1, lanes), jnp.int32),
            pltpu.SMEM((n_pages, 1, lanes), jnp.int32),
            pltpu.VMEM((n_pages, packed, width), jnp.float32),
            pltpu.VMEM((n_pages, n_patches, packed, width), jnp.float32),
            pltpu.VMEM((n_pages, n_patches, packed, width), jnp.float32),
            pltpu.VMEM((n_pages, up(2 * nq, 8), lanes), jnp.float32),
            pltpu.VMEM((n_pages, up(2 * nq, 8), lanes), jnp.float32),
            dma,
            dma((3,)),
            dma,
            dma((n_pages,)),
            dma,
            dma,
            dma((n_pages,)),
            dma,
            dma((n_pages,)),
            dma,
            dma((n_pages,)),
            dma,
            dma((n_pages,)),
            pltpu.SemaphoreType.REGULAR((n_pages,)),
        ],
        compiler_params=pltpu.CompilerParams(collective_id=0, has_side_effects=True),
    )(
        queries.reshape(nq * own_tokens, dim),
        gallery,
        page_rows,
        candidates,
    )


def solution(mesh):
    in_specs = (
        P(("groups", "pages"), "patches", None),
        P(("groups", "pages"), "patches", None),
        P("groups"),
        P(("groups", "pages"), None),
    )
    out_specs = P(("groups", "pages"), None)
    return jax.shard_map(body, mesh=mesh, in_specs=in_specs, out_specs=out_specs, check_vma=False)
```
